512 devices in a mesh: job: 2 (over y), chain: 16 (over z), pair: 8 (over x), pno: 2 (over core).
Axes of the slice: x: 8, y: 2, z: 16, core: 2. Of those that a mesh axis runs over, the one named last changes fastest.
The devices are a block of a 8x8x16 slice.
Arguments:
- amplitudes: bfloat16 [1536, 128, 128], P(('job', 'chain', 'pair'), 'pno'), parts along dimension 0, may hold values from -4 to 4
- integrals: bfloat16 [1536, 128, 128], P(('job', 'chain', 'pair'), 'pno'), parts along dimension 0, may hold values from -6 to 6
- intersections: bfloat16 [1536, 32, 128, 128], P(('job', 'chain', 'pair')), parts along dimension 0, may hold values from -0.5 to 0.5
- coupling: float32 [1536, 32], P(('job', 'chain', 'pair')), parts along dimension 0, may hold values from -4 to 4
- pno_energies: float32 [1536, 128], P(('job', 'chain', 'pair')), parts along dimension 0, may hold values from 0.3 to 3
- pair_shift: float32 [1536], P(('job', 'chain', 'pair')), parts along dimension 0, may hold values from -1.5 to -0.3
- ranks: int32 [1536], P(('job', 'chain', 'pair')), parts along dimension 0, may hold values from 24 to 128
- neighbours: int32 [1536, 32], P(('job', 'chain', 'pair')), parts along dimension 0, may hold values from 0 to 767, as said below
Outputs:
- final_amplitudes: bfloat16 [1536, 128, 128], P(('job', 'chain', 'pair'), 'pno'), parts along dimension 0
- residual_norms: float32 [6], P('job'), parts along dimension 0
The draws below stay inside these ranges and needn't reach their ends.
There are 2 independent parts, one for each index of `job`. The reference program is written for one: setup_inputs(seed, part) draws one part's arguments, and reference() takes and returns one part's arrays. A program takes and returns all parts, laid end to end along the dimension named above; each array names one. Nothing has to cross between parts.
Inputs may be any that keep to these rules, and one draw needn't show every extreme that they name: `neighbours`: every coupled pair of pair g lies in the fragment of g (pairs k * 48 to (k + 1) * 48 - 1 for k = g // 48) or in one of the two fragments beside it.
All inputs are finite; a program needn't handle non-finite values.
Results may differ from the reference program's by a relative error of at most 0.015.
Values may be sent and summed in bfloat16 or wider, within the bound.
No kernel may reach another device: no remote copies, remote signals or barrier semaphores. Data moves between devices by JAX's collectives and lax.ppermute only.
A program may use at most 64 MiB of HBM per device.

```python
import math
import jax
import jax.numpy as jnp
from jax import lax

R = 128
NB = 32
ITERS = 3
FRAG = 48
NPAIRS = 768


def draw_integrals(key, part):
    first, second = jax.random.split(jax.random.fold_in(key, 11))
    place = jnp.arange(NPAIRS, dtype=jnp.float32)
    scale = jnp.exp(jax.random.uniform(first, (NPAIRS,), minval=0.0, maxval=0.69)) * (1.0 + 9.0 * place / NPAIRS)
    base = jnp.clip(jax.random.normal(second, (NPAIRS, R, R)), -3.0, 3.0)
    return (0.1 * base * scale[:, None, None]).astype(jnp.bfloat16)


def draw_neighbours(key, part):
    first, second = jax.random.split(jax.random.fold_in(key, 23))
    offset = jax.random.randint(first, (NPAIRS, NB), -1, 2)
    home = jnp.arange(NPAIRS, dtype=jnp.int32) // FRAG
    target = jnp.clip(home[:, None] + offset, 0, NPAIRS // FRAG - 1)
    slot = jax.random.randint(second, (NPAIRS, NB), 0, FRAG)
    return (target * FRAG + slot).astype(jnp.int32)


def plant(entries, key, low, high):
    spot = [jax.random.randint(jax.random.fold_in(key, axis), (), 0, length) for axis, length in enumerate(entries.shape)]
    main_axis = entries.shape.index(max(entries.shape))
    next_to = spot[:main_axis] + [(spot[main_axis] + 1) % entries.shape[main_axis]] + spot[main_axis + 1:]
    return entries.at[tuple(spot)].set(low).at[tuple(next_to)].set(high)


def block_scale(rng, extent, cuts, low, high):
    def one(dim, shards_of):
        steps = jax.random.uniform(jax.random.fold_in(jax.random.fold_in(rng, 6), dim), (shards_of,), jnp.float32, low / len(cuts), high / len(cuts))
        return jnp.repeat(jnp.exp(steps), extent[dim] // shards_of).reshape((-1,) + (1,) * (len(extent) - dim - 1))

    loudness = one(*cuts[0])
    for cut in cuts[1:]:
        loudness = loudness * one(*cut)
    return loudness


def noise(rng, extent, deviation, reach, pieces=(), held_as=jnp.bfloat16):
    result = deviation * jax.random.normal(rng, extent, jnp.float32)
    if pieces:
        result = result * block_scale(rng, extent, pieces, -0.22, 0.18)
    return jnp.clip(result, -reach, reach).astype(held_as)


def setup_inputs(seed: int = 0, part: int = 0) -> dict:
    seeds = jax.random.split(jax.random.key(seed), 9)
    own_keys = jax.random.split(jax.random.fold_in(seeds[8], part), 9)
    amplitudes = noise(own_keys[0], (NPAIRS, R, R), 0.3, 4.0, ((0, 128), (1, 2)))
    integrals = draw_integrals(jax.random.fold_in(jax.random.fold_in(seeds[8], part), 71), part)
    intersections = noise(own_keys[2], (NPAIRS, NB, R, R), R ** -0.5, 0.5, ((0, 128),))
    coupling = noise(own_keys[3], (NPAIRS, NB), 1.0, 4.0, ((0, 128),), jnp.float32)
    pno_energies = jnp.clip(jnp.exp(math.log(3.0) - 2.3025851 * jax.random.uniform(own_keys[4], (NPAIRS, R), jnp.float32) ** block_scale(own_keys[4], (NPAIRS, R), ((0, 128),), -0.2, 0.2)), 0.3, 3.0)
    pair_shift = jnp.clip(-1.5 + 1.2 * jax.random.uniform(own_keys[5], (NPAIRS,), jnp.float32) ** block_scale(own_keys[5], (NPAIRS,), ((0, 128),), -0.2, 0.2), -1.5, -0.3)
    ranks = plant(jax.random.randint(own_keys[6], (NPAIRS,), 24, R + 1), jax.random.fold_in(own_keys[6], 1), 24, R).astype(jnp.int32)
    neighbours = draw_neighbours(jax.random.fold_in(jax.random.fold_in(seeds[8], part), 71), part)
    return dict(amplitudes=amplitudes, integrals=integrals, intersections=intersections, coupling=coupling, pno_energies=pno_energies, pair_shift=pair_shift, ranks=ranks, neighbours=neighbours)


def reference(amplitudes, integrals, intersections, coupling, pno_energies, pair_shift, ranks, neighbours):
    index = jnp.arange(R, dtype=jnp.int32)
    live = (index[None, :] < ranks[:, None]).astype(jnp.float32)
    mask = live[:, :, None] * live[:, None, :]
    denom = pno_energies[:, :, None] + pno_energies[:, None, :] - pair_shift[:, None, None]
    amps = (amplitudes.astype(jnp.float32) * mask).astype(jnp.bfloat16)
    ints = integrals.astype(jnp.float32)
    norms = []
    for step_no in range(ITERS):
        current = amps

        def pair_term(args):
            near, intersection, weights = args
            blocks = jnp.take(current, near, axis=0).astype(jnp.float32)
            over32 = intersection.astype(jnp.float32)
            proj = jnp.einsum('nab,nbc->nac', over32, blocks).astype(jnp.bfloat16)
            proj = lax.optimization_barrier(proj).astype(jnp.float32)
            terms = jnp.einsum('nac,nbc->nab', proj, over32)
            return jnp.einsum('n,nab->ab', weights, terms)
        coupled = lax.map(pair_term, (neighbours, intersections, coupling))
        amps32 = amps.astype(jnp.float32)
        resid = mask * (ints + coupled - denom * amps32)
        rms = jnp.sqrt(jnp.sum(resid * resid) / (NPAIRS * R * R))
        norms.append(rms)
        amps = (amps32 + resid / denom * (1.0 / (1.0 + rms))).astype(jnp.bfloat16)
    return (amps, jnp.stack(norms))
```

```python
import jax
import jax.numpy as jnp
from jax import lax
from jax.experimental import pallas as pl
from jax.experimental.pallas import tpu as pltpu
from jax.sharding import PartitionSpec as P

ITERS = 3
PRODUCTS = [(i, j) for i in range(ITERS) for j in range(i + 1)]


def shifted(value, axis, step):
    count = lax.axis_size(axis)
    pairs = [(i, i + step) for i in range(count) if 0 <= i + step < count]
    return lax.ppermute(value, axis, pairs)


def copies_of_all(value, axes):
    count = 1
    for axis in axes:
        count *= lax.axis_size(axis)
    copies = jnp.broadcast_to(value, (count, *value.shape))
    return lax.all_to_all(copies, axes, 0, 0, tiled=True)


def spread(piece):
    here = copies_of_all(piece, ("pair",))
    here = here.reshape(-1, *piece.shape[1:])
    return shifted(here, "chain", 1), here, shifted(here, "chain", -1)


def live_cells(rank, first, half, width):
    rows = first + lax.broadcasted_iota(jnp.int32, (half, width), 0)
    columns = lax.broadcasted_iota(jnp.int32, (half, width), 1)
    return (rows < rank) & (columns < rank)


def start_kernel(side, ranks, amplitudes, own):
    count, half, width = amplitudes.shape
    for g in range(count):
        live = live_cells(ranks[g], side[0] * half, half, width)
        block = jnp.where(live, amplitudes[g].astype(jnp.float32), 0.0)
        own[g] = block.astype(jnp.bfloat16)


def masked(side, ranks, amplitudes):
    return pl.pallas_call(
        start_kernel,
        grid_spec=pltpu.PrefetchScalarGridSpec(
            num_scalar_prefetch=2,
            grid=(1,),
            in_specs=[pl.BlockSpec(amplitudes.shape, lambda i, *_: (0, 0, 0))],
            out_specs=pl.BlockSpec(amplitudes.shape, lambda i, *_: (0, 0, 0)),
        ),
        out_shape=jax.ShapeDtypeStruct(amplitudes.shape, jnp.bfloat16),
        name="masked",
    )(side, ranks, amplitudes)


def couple_kernel(slots, side, weights, low, here, high, over, out, window, stack):
    pair = pl.program_id(0)
    terms, width = over.shape[1], over.shape[2]
    half = here.shape[1]
    first = pl.multiple_of(side[0] * half, half)

    @pl.when(pair == 0)
    def _():
        frag = here.shape[0]
        window[0:frag] = low[...]
        window[frag : 2 * frag] = here[...]
        window[2 * frag : 3 * frag] = high[...]
        stack[...] = jnp.zeros_like(stack)

    for n in range(terms):
        block = window[slots[pair * terms + n]]
        right = lax.dot_general(
            block, over[0, n], (((1,), (1,)), ((), ())), preferred_element_type=jnp.float32
        )
        right = (right * weights[pair * terms + n]).astype(jnp.bfloat16)
        stack[pl.ds(pl.multiple_of(n * width + first, half), half), :] = right
    left = jnp.concatenate([over[0, n] for n in range(terms)], axis=1)
    both = jnp.dot(left, stack[...], preferred_element_type=jnp.float32)
    out[0, 0] = both[:half]
    out[1, 0] = both[half:]


def couple(slots, side, weights, low, here, high, over):
    count, terms, width, _ = over.shape
    frag, half, _ = here.shape
    whole = pl.BlockSpec((frag, half, width), lambda g, *_: (0, 0, 0))
    grid_spec = pltpu.PrefetchScalarGridSpec(
        num_scalar_prefetch=3,
        grid=(count,),
        in_specs=[
            whole,
            whole,
            whole,
            pl.BlockSpec((1, terms, width, width), lambda g, *_: (g, 0, 0, 0)),
        ],
        out_specs=pl.BlockSpec((2, 1, half, width), lambda g, *_: (0, g, 0, 0)),
        scratch_shapes=[
            pltpu.VMEM((3 * frag, half, width), jnp.bfloat16),
            pltpu.VMEM((terms * width, width), jnp.bfloat16),
        ],
    )
    return pl.pallas_call(
        couple_kernel,
        grid_spec=grid_spec,
        out_shape=jax.ShapeDtypeStruct((2, count, half, width), jnp.float32),
        compiler_params=pltpu.CompilerParams(
            dimension_semantics=("arbitrary",), vmem_limit_bytes=24 * 1024 * 1024
        ),
        name="couple",
    )(slots, side, weights, low, here, high, over)


def products_kernel(scale, parts, mask, *refs):
    held, (last, sums) = refs[:-2], refs[-2:]
    last[...] = mask[...] * (parts[0] + parts[1]) - held[-1][...]
    terms = [ref[...] * scale for ref in held] + [last[...] * scale]
    lane = lax.broadcasted_iota(jnp.int32, sums.shape, 1)
    row = jnp.zeros(sums.shape, jnp.float32)
    for place, (i, j) in enumerate(PRODUCTS):
        row = jnp.where(lane == place, jnp.sum(terms[i] * terms[j]), row)
    sums[...] = row


def products(scale, parts, mask, held):
    shape = mask.shape
    return pl.pallas_call(
        lambda *refs: products_kernel(scale, *refs),
        out_shape=(
            jax.ShapeDtypeStruct(shape, jnp.float32),
            jax.ShapeDtypeStruct((1, shape[-1]), jnp.float32),
        ),
        name="products",
    )(parts, mask, *held)


def finish_kernel(copies, own, denom, *refs):
    terms, (amps, norms) = refs[:-2], refs[-2:]
    total = jnp.sum(copies[...], axis=0)
    gram = {}
    for place, (i, j) in enumerate(PRODUCTS):
        gram[i, j] = gram[j, i] = total[:, place : place + 1]
    one = jnp.ones_like(gram[0, 0])
    shares = [one] + [jnp.zeros_like(one)] * (ITERS - 1)
    sums = [jnp.zeros_like(one)] * ITERS
    for step_no in range(ITERS):
        square = jnp.zeros_like(one)
        for i in range(step_no + 1):
            for j in range(step_no + 1):
                square = square + (shares[i] * gram[i, j]) * shares[j]
        rms = jnp.sqrt(jnp.maximum(square, 0.0))
        norms[step_no] = rms[0, 0]
        factor = 1.0 / (1.0 + rms)
        sums = [held + factor * share for held, share in zip(sums, shares, strict=True)]
        shares = [shares[0]] + [
            shares[i] + factor * shares[i - 1] for i in range(1, ITERS)
        ]
    change = sum(held * ref[...].reshape(-1, own.shape[-1]) for held, ref in zip(sums, terms, strict=True))
    change = change.reshape(own.shape)
    amps[...] = (own[...].astype(jnp.float32) + change / denom[...]).astype(jnp.bfloat16)


def finish(copies, own, denom, terms):
    return pl.pallas_call(
        finish_kernel,
        out_shape=(
            jax.ShapeDtypeStruct(own.shape, jnp.bfloat16),
            jax.ShapeDtypeStruct((ITERS,), jnp.float32),
        ),
        out_specs=(pl.BlockSpec(memory_space=pltpu.VMEM), pl.BlockSpec(memory_space=pltpu.SMEM)),
        name="finish",
    )(copies, own, denom, *terms)


def per_device(
    amplitudes, integrals, intersections, coupling, pno_energies, pair_shift, ranks, neighbours
):
    count, half, width = amplitudes.shape
    chain_pos = lax.axis_index("chain")
    side = lax.axis_index("pno")
    first_row = side * half
    frag = count * lax.axis_size("pair")
    cells = frag * lax.axis_size("chain") * width * width
    sides = jnp.reshape(side, (1,)).astype(jnp.int32)
    own = masked(sides, ranks, amplitudes)
    columns = jnp.arange(width, dtype=jnp.int32)
    rows_here = first_row + jnp.arange(half, dtype=jnp.int32)
    live_cols = columns[None, :] < ranks[:, None]
    live_rows = rows_here[None, :] < ranks[:, None]
    mask = (live_rows[:, :, None] & live_cols[:, None, :]).astype(jnp.float32)
    energy_rows = lax.dynamic_slice_in_dim(pno_energies, first_row, half, 1)
    denom = energy_rows[:, :, None] + pno_energies[:, None, :] - pair_shift[:, None, None]
    slots = (neighbours - (chain_pos - 1) * frag).reshape(-1)
    weights = coupling.reshape(-1)
    over = pltpu.with_memory_space_constraint(intersections, pltpu.HBM)

    def coupled_parts(piece):
        low, here, high = spread(piece)
        parts = couple(slots, sides, weights, low, here, high, over)
        return lax.all_to_all(parts, "pno", 0, 0, tiled=True)

    parts = coupled_parts(own)
    ints = integrals.astype(jnp.float32)
    terms = [mask * (ints + (parts[0] + parts[1]) - denom * own.astype(jnp.float32))]
    for step_no in range(1, ITERS):
        parts = coupled_parts((terms[-1] / denom).astype(jnp.bfloat16))
        if step_no + 1 < ITERS:
            terms.append(mask * (parts[0] + parts[1]) - terms[-1])
    last, sums = products(cells**-0.5, parts, mask, terms)
    sums = jnp.sum(copies_of_all(sums, ("pair", "pno")), axis=0, keepdims=True)[0]
    return tuple(finish(copies_of_all(sums, ("chain",)), own, denom, terms + [last]))


def solution(mesh):
    in_specs = (
        P(("job", "chain", "pair"), "pno", None),
        P(("job", "chain", "pair"), "pno", None),
        P(("job", "chain", "pair"), None, None, None),
        P(("job", "chain", "pair"), None),
        P(("job", "chain", "pair"), None),
        P(("job", "chain", "pair")),
        P(("job", "chain", "pair")),
        P(("job", "chain", "pair"), None),
    )
    out_specs = (P(("job", "chain", "pair"), "pno", None), P("job"))
    return jax.shard_map(
        per_device, mesh=mesh, in_specs=in_specs, out_specs=out_specs, check_vma=False
    )
```

```python
import jax
import jax.numpy as jnp
from jax import lax
from jax.experimental import pallas as pl
from jax.experimental.pallas import tpu as pltpu
from jax.sharding import PartitionSpec as P

ITERS = 3
PRODUCTS = [(i, j) for i in range(ITERS) for j in range(i + 1)]


def shifted(value, axis, step, around=False):
    count = lax.axis_size(axis)
    pairs = [(i, (i + step) % count) for i in range(count) if around or 0 <= i + step < count]
    return lax.ppermute(value, axis, pairs)


def copies_of_all(value, axes):
    count = 1
    for axis in axes:
        count *= lax.axis_size(axis)
    copies = jnp.broadcast_to(value, (count, *value.shape))
    return lax.all_to_all(copies, axes, 0, 0, tiled=True)


def spread(copies):
    count = lax.axis_size("pair")
    groups = [list(range(first, count, 2)) for first in range(2)]
    near = lax.all_to_all(copies, "pair", 0, 0, tiled=True, axis_index_groups=groups)
    near = near.reshape(-1, *copies.shape[2:])
    low, high = shifted(near, "chain", 1), shifted(near, "chain", -1)
    other = shifted(near, "pair", 1, around=True)
    low_other = shifted(low, "pair", 1, around=True)
    high_other = shifted(high, "pair", -1, around=True)
    return low, low_other, near, other, high, high_other


def live_cells(rank, first, half, width):
    rows = first + lax.broadcasted_iota(jnp.int32, (half, width), 0)
    columns = lax.broadcasted_iota(jnp.int32, (half, width), 1)
    return (rows < rank) & (columns < rank)


def start_kernel(side, ranks, amplitudes, own, copies):
    count, half, width = amplitudes.shape
    for g in range(count):
        live = live_cells(ranks[g], side[0] * half, half, width)
        block = jnp.where(live, amplitudes[g].astype(jnp.float32), 0.0)
        block = block.astype(jnp.bfloat16)
        own[g] = block
        for copy in range(copies.shape[0]):
            copies[copy, g] = block


def masked(side, ranks, amplitudes, count):
    shape = amplitudes.shape
    return pl.pallas_call(
        start_kernel,
        grid_spec=pltpu.PrefetchScalarGridSpec(
            num_scalar_prefetch=2,
            grid=(1,),
            in_specs=[pl.BlockSpec(shape, lambda i, *_: (0, 0, 0))],
            out_specs=[
                pl.BlockSpec(shape, lambda i, *_: (0, 0, 0)),
                pl.BlockSpec((count, *shape), lambda i, *_: (0, 0, 0, 0)),
            ],
        ),
        out_shape=(
            jax.ShapeDtypeStruct(shape, jnp.bfloat16),
            jax.ShapeDtypeStruct((count, *shape), jnp.bfloat16),
        ),
        name="masked",
    )(side, ranks, amplitudes)


def arrange_kernel(side, after, over, across, halves):
    terms, width = over.shape[1], over.shape[2]
    half = width // 2
    row = lax.broadcasted_iota(jnp.int32, (width, width), 0)
    lane = lax.broadcasted_iota(jnp.int32, (width, width), 1)
    first = side[0] * half
    even = ((lane < half) & (row == lane + first)).astype(jnp.bfloat16)
    odd = ((lane >= half) & (row == lane - half + first)).astype(jnp.bfloat16)
    picks = jnp.concatenate([even, odd], axis=0)
    for n in range(0, terms, 2):
        two = jnp.concatenate([over[0, n], over[0, n + 1]], axis=1)
        picked = jnp.dot(two, picks, preferred_element_type=jnp.float32).astype(jnp.bfloat16)
        halves[0, :, n * half : (n + 2) * half] = picked
    for n in range(terms):
        across[0, n] = over[0, n].T


def arrange(side, after, over):
    count, terms, width, _ = over.shape
    across = (count, terms, width, width)
    halves = (count, width, terms * width // 2)
    return pl.pallas_call(
        arrange_kernel,
        grid_spec=pltpu.PrefetchScalarGridSpec(
            num_scalar_prefetch=1,
            grid=(count,),
            in_specs=[
                pl.BlockSpec((1, *after.shape[1:]), lambda g, *_: (0, 0, 0)),
                pl.BlockSpec((1, *over.shape[1:]), lambda g, *_: (g, 0, 0, 0)),
            ],
            out_specs=[
                pl.BlockSpec((1, *across[1:]), lambda g, *_: (g, 0, 0, 0)),
                pl.BlockSpec((1, *halves[1:]), lambda g, *_: (g, 0, 0)),
            ],
        ),
        out_shape=(
            pltpu.VMEM(across, over.dtype),
            pltpu.VMEM(halves, over.dtype),
        ),
        compiler_params=pltpu.CompilerParams(
            dimension_semantics=("arbitrary",), vmem_limit_bytes=24 * 1024 * 1024
        ),
        cost_estimate=pl.CostEstimate(flops=10**9, transcendentals=0, bytes_accessed=3 * over.size),
        name="arrange",
    )(side, after, over)


def couple_kernel(slots, weights, across, halves, *refs):
    pieces, (out, window, stacks) = refs[:-3], refs[-3:]
    count, terms, width, _ = across.shape
    size, half, _ = pieces[0].shape
    for place, piece in enumerate(pieces):
        window[place * size : (place + 1) * size] = piece[...]

    def right_side(g, stack):
        for n in range(terms):
            place = g * terms + n
            right = jnp.dot(
                window[slots[place]], across[g, n], preferred_element_type=jnp.float32
            )
            stack[n * half : (n + 1) * half] = (right * weights[place]).astype(jnp.bfloat16)

    def left_side(g, stack):
        both = jnp.dot(halves[g], stack[...], preferred_element_type=jnp.float32)
        out[0, g] = both[:half]
        out[1, g] = both[half:]

    right_side(0, stacks.at[0])

    def step(g, carry):
        right_side(g, stacks.at[lax.rem(g, 2)])
        left_side(g - 1, stacks.at[lax.rem(g - 1, 2)])
        return carry

    lax.fori_loop(1, count, step, 0)
    left_side(count - 1, stacks.at[(count - 1) % 2])


def couple(slots, weights, across, halves, pieces):
    count, terms, width, _ = across.shape
    size, half, _ = pieces[0].shape
    inside = pl.BlockSpec(memory_space=pltpu.VMEM)
    scalars = pl.BlockSpec(memory_space=pltpu.SMEM)
    return pl.pallas_call(
        couple_kernel,
        in_specs=[scalars, scalars] + [inside] * (2 + len(pieces)),
        out_specs=inside,
        out_shape=jax.ShapeDtypeStruct((2, count, half, width), jnp.float32),
        scratch_shapes=[
            pltpu.VMEM((len(pieces) * size, half, width), jnp.bfloat16),
            pltpu.VMEM((2, terms * half, width), jnp.bfloat16),
        ],
        compiler_params=pltpu.CompilerParams(vmem_limit_bytes=24 * 1024 * 1024),
        name="couple",
    )(slots, weights, across, halves, *pieces)


def products_kernel(scale, parts, mask, *refs):
    held, (last, sums) = refs[:-2], refs[-2:]
    last[...] = mask[...] * (parts[0] + parts[1]) - held[-1][...]
    terms = [ref[...] * scale for ref in held] + [last[...] * scale]
    lane = lax.broadcasted_iota(jnp.int32, sums.shape, 1)
    row = jnp.zeros(sums.shape, jnp.float32)
    for place, (i, j) in enumerate(PRODUCTS):
        row = jnp.where(lane == place, jnp.sum(terms[i] * terms[j]), row)
    sums[...] = row


def products(scale, parts, mask, held):
    shape = mask.shape
    return pl.pallas_call(
        lambda *refs: products_kernel(scale, *refs),
        out_shape=(
            jax.ShapeDtypeStruct(shape, jnp.float32),
            jax.ShapeDtypeStruct((1, shape[-1]), jnp.float32),
        ),
        name="products",
    )(parts, mask, *held)


def finish_kernel(copies, own, denom, *refs):
    terms, (amps, norms) = refs[:-2], refs[-2:]
    total = jnp.sum(copies[...], axis=0)
    gram = {}
    for place, (i, j) in enumerate(PRODUCTS):
        gram[i, j] = gram[j, i] = total[:, place : place + 1]
    one = jnp.ones_like(gram[0, 0])
    shares = [one] + [jnp.zeros_like(one)] * (ITERS - 1)
    sums = [jnp.zeros_like(one)] * ITERS
    for step_no in range(ITERS):
        square = jnp.zeros_like(one)
        for i in range(step_no + 1):
            for j in range(step_no + 1):
                square = square + (shares[i] * gram[i, j]) * shares[j]
        rms = jnp.sqrt(jnp.maximum(square, 0.0))
        norms[step_no] = rms[0, 0]
        factor = 1.0 / (1.0 + rms)
        sums = [held + factor * share for held, share in zip(sums, shares, strict=True)]
        shares = [shares[0]] + [
            shares[i] + factor * shares[i - 1] for i in range(1, ITERS)
        ]
    change = sum(held * ref[...].reshape(-1, own.shape[-1]) for held, ref in zip(sums, terms, strict=True))
    change = change.reshape(own.shape)
    amps[...] = (own[...].astype(jnp.float32) + change / denom[...]).astype(jnp.bfloat16)


def finish(copies, own, denom, terms):
    return pl.pallas_call(
        finish_kernel,
        out_shape=(
            jax.ShapeDtypeStruct(own.shape, jnp.bfloat16),
            jax.ShapeDtypeStruct((ITERS,), jnp.float32),
        ),
        out_specs=(pl.BlockSpec(memory_space=pltpu.VMEM), pl.BlockSpec(memory_space=pltpu.SMEM)),
        name="finish",
    )(copies, own, denom, *terms)


def per_device(
    amplitudes, integrals, intersections, coupling, pno_energies, pair_shift, ranks, neighbours
):
    count, half, width = amplitudes.shape
    chain_pos = lax.axis_index("chain")
    side = lax.axis_index("pno")
    first_row = side * half
    frag = count * lax.axis_size("pair")
    cells = frag * lax.axis_size("chain") * width * width
    sides = jnp.reshape(side, (1,)).astype(jnp.int32)
    near = lax.axis_size("pair") // 2
    own, copies = masked(sides, ranks, amplitudes, near)
    columns = jnp.arange(width, dtype=jnp.int32)
    rows_here = first_row + jnp.arange(half, dtype=jnp.int32)
    live_cols = columns[None, :] < ranks[:, None]
    live_rows = rows_here[None, :] < ranks[:, None]
    mask = (live_rows[:, :, None] & live_cols[:, None, :]).astype(jnp.float32)
    energy_rows = lax.dynamic_slice_in_dim(pno_energies, first_row, half, 1)
    denom = energy_rows[:, :, None] + pno_energies[:, None, :] - pair_shift[:, None, None]
    within = neighbours % frag
    place = within // count
    turn = (place - lax.axis_index("pair")) % 2
    piece_no = 2 * (neighbours // frag - chain_pos + 1) + turn
    slots = ((piece_no * near + place // 2) * count + within % count).reshape(-1)
    weights = coupling.reshape(-1)
    over = pltpu.with_memory_space_constraint(intersections, pltpu.HBM)

    kept = []

    def coupled_parts(copies):
        pieces = spread(copies)
        if not kept:
            kept.extend(arrange(sides, pieces[2], over))
        parts = couple(slots, weights, *kept, pieces)
        return lax.all_to_all(parts, "pno", 0, 0, tiled=True)

    parts = coupled_parts(copies)
    ints = integrals.astype(jnp.float32)
    terms = [mask * (ints + (parts[0] + parts[1]) - denom * own.astype(jnp.float32))]
    for step_no in range(1, ITERS):
        piece = (terms[-1] / denom).astype(jnp.bfloat16)
        parts = coupled_parts(jnp.broadcast_to(piece, (near, *piece.shape)))
        if step_no + 1 < ITERS:
            terms.append(mask * (parts[0] + parts[1]) - terms[-1])
    last, sums = products(cells**-0.5, parts, mask, terms)
    sums = jnp.sum(copies_of_all(sums, ("chain", "pno")), axis=0)
    return tuple(finish(copies_of_all(sums, ("pair",)), own, denom, terms + [last]))


def solution(mesh):
    in_specs = (
        P(("job", "chain", "pair"), "pno", None),
        P(("job", "chain", "pair"), "pno", None),
        P(("job", "chain", "pair"), None, None, None),
        P(("job", "chain", "pair"), None),
        P(("job", "chain", "pair"), None),
        P(("job", "chain", "pair")),
        P(("job", "chain", "pair")),
        P(("job", "chain", "pair"), None),
    )
    out_specs = (P(("job", "chain", "pair"), "pno", None), P("job"))
    return jax.shard_map(
        per_device, mesh=mesh, in_specs=in_specs, out_specs=out_specs, check_vma=False
    )
```

```python
import jax
import jax.numpy as jnp
from jax import lax
from jax.experimental import pallas as pl
from jax.experimental.pallas import tpu as pltpu
from jax.sharding import PartitionSpec as P

ITERS = 3
PRODUCTS = [(i, j) for i in range(ITERS) for j in range(i + 1)]


def swapped(value, axis, first, around):
    count = lax.axis_size(axis)
    pairs = []
    for left in range(first, count, 2):
        if left + 1 < count or around:
            right = (left + 1) % count
            pairs += [(left, right), (right, left)]
    return lax.ppermute(value, axis, pairs)


def joined(value, step, first):
    count = lax.axis_size("pair")
    groups = []
    for start in range(first, first + count, 2 * step):
        for parity in range(step):
            left, right = (start + parity) % count, (start + step + parity) % count
            groups.append(sorted([left, right]))
    return lax.all_gather(value, "pair", axis=0, tiled=True, axis_index_groups=groups)


def spread(piece):
    near = joined(joined(piece, 2, 0), 2, 2)
    ahead = swapped(near, "chain", 0, False)
    behind = swapped(near, "chain", 1, False)
    other = swapped(near, "pair", 0, True)
    ahead_other = swapped(ahead, "pair", 1, True)
    behind_other = swapped(behind, "pair", 0, True)
    return near, other, ahead, ahead_other, behind, behind_other


def live_cells(rank, first, half, width):
    rows = first + lax.broadcasted_iota(jnp.int32, (half, width), 0)
    columns = lax.broadcasted_iota(jnp.int32, (half, width), 1)
    return (rows < rank) & (columns < rank)


def start_kernel(side, ranks, amplitudes, own):
    count, half, width = amplitudes.shape
    for g in range(count):
        live = live_cells(ranks[g], side[0] * half, half, width)
        block = jnp.where(live, amplitudes[g].astype(jnp.float32), 0.0)
        own[g] = block.astype(jnp.bfloat16)


def masked(side, ranks, amplitudes):
    shape = amplitudes.shape
    return pl.pallas_call(
        start_kernel,
        grid_spec=pltpu.PrefetchScalarGridSpec(
            num_scalar_prefetch=2,
            grid=(1,),
            in_specs=[pl.BlockSpec(shape, lambda i, *_: (0, 0, 0))],
            out_specs=pl.BlockSpec(shape, lambda i, *_: (0, 0, 0)),
        ),
        out_shape=jax.ShapeDtypeStruct(shape, jnp.bfloat16),
        compiler_params=pltpu.CompilerParams(vmem_limit_bytes=8 * 1024 * 1024),
        name="masked",
    )(side, ranks, amplitudes)


def arrange_kernel(side, after, over, across, halves):
    terms, width = over.shape[1], over.shape[2]
    half = width // 2
    row = lax.broadcasted_iota(jnp.int32, (width, width), 0)
    lane = lax.broadcasted_iota(jnp.int32, (width, width), 1)
    first = side[0] * half
    even = ((lane < half) & (row == lane + first)).astype(jnp.bfloat16)
    odd = ((lane >= half) & (row == lane - half + first)).astype(jnp.bfloat16)
    picks = jnp.concatenate([even, odd], axis=0)
    for n in range(0, terms, 2):
        two = jnp.concatenate([over[0, n], over[0, n + 1]], axis=1)
        picked = jnp.dot(two, picks, preferred_element_type=jnp.float32).astype(jnp.bfloat16)
        halves[0, :, n * half : (n + 2) * half] = picked
    for n in range(terms):
        across[0, n] = over[0, n].T


def arrange(side, after, over):
    count, terms, width, _ = over.shape
    across = (count, terms, width, width)
    halves = (count, width, terms * width // 2)
    return pl.pallas_call(
        arrange_kernel,
        grid_spec=pltpu.PrefetchScalarGridSpec(
            num_scalar_prefetch=1,
            grid=(count,),
            in_specs=[
                pl.BlockSpec((1, *after.shape[1:]), lambda g, *_: (0, 0, 0)),
                pl.BlockSpec((1, *over.shape[1:]), lambda g, *_: (g, 0, 0, 0)),
            ],
            out_specs=[
                pl.BlockSpec((1, *across[1:]), lambda g, *_: (g, 0, 0, 0)),
                pl.BlockSpec((1, *halves[1:]), lambda g, *_: (g, 0, 0)),
            ],
        ),
        out_shape=(
            pltpu.VMEM(across, over.dtype),
            pltpu.VMEM(halves, over.dtype),
        ),
        compiler_params=pltpu.CompilerParams(
            dimension_semantics=("arbitrary",), vmem_limit_bytes=24 * 1024 * 1024
        ),
        cost_estimate=pl.CostEstimate(flops=10**9, transcendentals=0, bytes_accessed=3 * over.size),
        name="arrange",
    )(side, after, over)


def couple_kernel(side, slots, weights, across, halves, *refs):
    pieces, (mine, theirs, window, stacks) = refs[:-4], refs[-4:]
    count, terms, width, _ = across.shape
    size, half, _ = pieces[0].shape
    for place, piece in enumerate(pieces):
        window[place * size : (place + 1) * size] = piece[...]

    def right_side(g, stack):
        for n in range(terms):
            place = g * terms + n
            right = jnp.dot(
                window[slots[place]], across[g, n], preferred_element_type=jnp.float32
            )
            stack[n * half : (n + 1) * half] = (right * weights[place]).astype(jnp.bfloat16)

    def left_side(g, stack):
        both = jnp.dot(halves[g], stack[...], preferred_element_type=jnp.float32)
        upper = side[0] == 0
        mine[g] = jnp.where(upper, both[:half], both[half:])
        theirs[g] = jnp.where(upper, both[half:], both[:half])

    right_side(0, stacks.at[0])

    def step(g, carry):
        right_side(g, stacks.at[lax.rem(g, 2)])
        left_side(g - 1, stacks.at[lax.rem(g - 1, 2)])
        return carry

    lax.fori_loop(1, count, step, 0)
    left_side(count - 1, stacks.at[(count - 1) % 2])


def couple(side, slots, weights, across, halves, pieces):
    count, terms, width, _ = across.shape
    size, half, _ = pieces[0].shape
    inside = pl.BlockSpec(memory_space=pltpu.VMEM)
    scalars = pl.BlockSpec(memory_space=pltpu.SMEM)
    return pl.pallas_call(
        couple_kernel,
        in_specs=[scalars] * 3 + [inside] * (2 + len(pieces)),
        out_specs=[inside] * 2,
        out_shape=[jax.ShapeDtypeStruct((count, half, width), jnp.float32)] * 2,
        scratch_shapes=[
            pltpu.VMEM((len(pieces) * size, half, width), jnp.bfloat16),
            pltpu.VMEM((2, terms * half, width), jnp.bfloat16),
        ],
        compiler_params=pltpu.CompilerParams(vmem_limit_bytes=24 * 1024 * 1024),
        name="couple",
    )(side, slots, weights, across, halves, *pieces)


def products_kernel(scale, mine, theirs, mask, *refs):
    held, (last, sums) = refs[:-2], refs[-2:]
    last[...] = mask[...] * (mine[...] + theirs[...]) - held[-1][...]
    terms = [ref[...] * scale for ref in held] + [last[...] * scale]
    lane = lax.broadcasted_iota(jnp.int32, sums.shape, 2)
    row = jnp.zeros(sums.shape, jnp.float32)
    for place, (i, j) in enumerate(PRODUCTS):
        row = jnp.where(lane == place, jnp.sum(terms[i] * terms[j]), row)
    sums[...] = row


def products(scale, mine, theirs, mask, held, count):
    shape = mask.shape
    inside = pl.BlockSpec(memory_space=pltpu.VMEM)
    return pl.pallas_call(
        lambda *refs: products_kernel(scale, *refs),
        in_specs=[inside] * (3 + len(held)),
        out_specs=(inside, inside),
        out_shape=(
            jax.ShapeDtypeStruct(shape, jnp.float32),
            jax.ShapeDtypeStruct((count, 1, shape[-1]), jnp.float32),
        ),
        compiler_params=pltpu.CompilerParams(vmem_limit_bytes=8 * 1024 * 1024),
        name="products",
    )(mine, theirs, mask, *held)


def finish_kernel(copies, own, denom, *refs):
    terms, (amps, norms) = refs[:-2], refs[-2:]
    total = jnp.sum(copies[...], axis=0)
    gram = {}
    for place, (i, j) in enumerate(PRODUCTS):
        gram[i, j] = gram[j, i] = total[:, place : place + 1]
    one = jnp.ones_like(gram[0, 0])
    shares = [one] + [jnp.zeros_like(one)] * (ITERS - 1)
    sums = [jnp.zeros_like(one)] * ITERS
    for step_no in range(ITERS):
        square = jnp.zeros_like(one)
        for i in range(step_no + 1):
            for j in range(step_no + 1):
                square = square + (shares[i] * gram[i, j]) * shares[j]
        rms = jnp.sqrt(jnp.maximum(square, 0.0))
        norms[step_no] = rms[0, 0]
        factor = 1.0 / (1.0 + rms)
        sums = [held + factor * share for held, share in zip(sums, shares, strict=True)]
        shares = [shares[0]] + [
            shares[i] + factor * shares[i - 1] for i in range(1, ITERS)
        ]
    change = sum(held * ref[...].reshape(-1, own.shape[-1]) for held, ref in zip(sums, terms, strict=True))
    change = change.reshape(own.shape)
    amps[...] = (own[...].astype(jnp.float32) + change / denom[...]).astype(jnp.bfloat16)


def finish(copies, own, denom, terms):
    return pl.pallas_call(
        finish_kernel,
        out_shape=(
            jax.ShapeDtypeStruct(own.shape, jnp.bfloat16),
            jax.ShapeDtypeStruct((ITERS,), jnp.float32),
        ),
        in_specs=[pl.BlockSpec(memory_space=pltpu.VMEM)] * (3 + len(terms)),
        out_specs=(pl.BlockSpec(memory_space=pltpu.VMEM), pl.BlockSpec(memory_space=pltpu.SMEM)),
        compiler_params=pltpu.CompilerParams(vmem_limit_bytes=8 * 1024 * 1024),
        name="finish",
    )(copies, own, denom, *terms)


def per_device(
    amplitudes, integrals, intersections, coupling, pno_energies, pair_shift, ranks, neighbours
):
    count, half, width = amplitudes.shape
    chain_pos = lax.axis_index("chain")
    side = lax.axis_index("pno")
    first_row = side * half
    frag = count * lax.axis_size("pair")
    cells = frag * lax.axis_size("chain") * width * width
    sides = jnp.reshape(side, (1,)).astype(jnp.int32)
    own = masked(sides, ranks, amplitudes)
    columns = jnp.arange(width, dtype=jnp.int32)
    rows_here = first_row + jnp.arange(half, dtype=jnp.int32)
    live_cols = columns[None, :] < ranks[:, None]
    live_rows = rows_here[None, :] < ranks[:, None]
    mask = (live_rows[:, :, None] & live_cols[:, None, :]).astype(jnp.float32)
    energy_rows = lax.dynamic_slice_in_dim(pno_energies, first_row, half, 1)
    denom = energy_rows[:, :, None] + pno_energies[:, None, :] - pair_shift[:, None, None]
    within = neighbours % frag
    place = within // count
    turn = (place - lax.axis_index("pair")) % 2
    offset = neighbours // frag - chain_pos
    facing = 1 - 2 * (chain_pos % 2)
    piece_no = 2 * jnp.where(offset == 0, 0, jnp.where(offset == facing, 1, 2)) + turn
    near = lax.axis_size("pair") // 2
    slots = ((piece_no * near + place // 2) * count + within % count).reshape(-1)
    weights = coupling.reshape(-1)
    over = pltpu.with_memory_space_constraint(intersections, pltpu.HBM)

    kept = []

    def coupled_parts(piece):
        pieces = spread(piece)
        if not kept:
            kept.extend(arrange(sides, pieces[0], over))
        mine, theirs = couple(sides, slots, weights, *kept, pieces)
        return mine, swapped(theirs, "pno", 0, False)

    mine, theirs = coupled_parts(own)
    ints = integrals.astype(jnp.float32)
    terms = [mask * (ints + (mine + theirs) - denom * own.astype(jnp.float32))]
    for step_no in range(1, ITERS):
        mine, theirs = coupled_parts((terms[-1] / denom).astype(jnp.bfloat16))
        if step_no + 1 < ITERS:
            terms.append(mask * (mine + theirs) - terms[-1])
    lines = lax.axis_size("chain") * lax.axis_size("pno")
    last, sums = products(cells**-0.5, mine, theirs, mask, terms, lines)
    sums = lax.all_to_all(sums, ("chain", "pno"), 0, 0, tiled=True)
    sums = jnp.broadcast_to(jnp.sum(sums, axis=0), (lax.axis_size("pair"), 1, width))
    sums = lax.all_to_all(sums, "pair", 0, 0, tiled=True)
    return tuple(finish(sums, own, denom, terms + [last]))


def solution(mesh):
    in_specs = (
        P(("job", "chain", "pair"), "pno", None),
        P(("job", "chain", "pair"), "pno", None),
        P(("job", "chain", "pair"), None, None, None),
        P(("job", "chain", "pair"), None),
        P(("job", "chain", "pair"), None),
        P(("job", "chain", "pair")),
        P(("job", "chain", "pair")),
        P(("job", "chain", "pair"), None),
    )
    out_specs = (P(("job", "chain", "pair"), "pno", None), P("job"))
    return jax.shard_map(
        per_device, mesh=mesh, in_specs=in_specs, out_specs=out_specs, check_vma=False
    )
```

```python
import jax
import jax.numpy as jnp
from jax import lax
from jax.experimental import pallas as pl
from jax.experimental.pallas import tpu as pltpu
from jax.sharding import PartitionSpec as P

ITERS = 3
PRODUCTS = [(i, j) for i in range(ITERS) for j in range(i + 1)]


def shifted(value, axis, step, around=False):
    count = lax.axis_size(axis)
    pairs = [(i, (i + step) % count) for i in range(count) if around or 0 <= i + step < count]
    return lax.ppermute(value, axis, pairs)


def joined(value, step, first):
    count = lax.axis_size("pair")
    groups = []
    for start in range(first, first + count, 2 * step):
        for parity in range(step):
            left, right = (start + parity) % count, (start + step + parity) % count
            groups.append(sorted([left, right]))
    both = jnp.broadcast_to(value, (2, *value.shape))
    both = lax.all_to_all(both, "pair", 0, 0, tiled=True, axis_index_groups=groups)
    return both.reshape(-1, *value.shape[1:])


def spread(piece):
    near = joined(joined(piece, 2, 0), 2, 2)
    low, high = shifted(near, "chain", 1), shifted(near, "chain", -1)
    other = shifted(near, "pair", -1, around=True)
    low_other = shifted(low, "pair", 1, around=True)
    high_other = shifted(high, "pair", -1, around=True)
    return low, low_other, near, other, high, high_other


def live_cells(rank, first, half, width):
    rows = first + lax.broadcasted_iota(jnp.int32, (half, width), 0)
    columns = lax.broadcasted_iota(jnp.int32, (half, width), 1)
    return (rows < rank) & (columns < rank)


def start_kernel(side, ranks, amplitudes, own):
    count, half, width = amplitudes.shape
    for g in range(count):
        live = live_cells(ranks[g], side[0] * half, half, width)
        block = jnp.where(live, amplitudes[g].astype(jnp.float32), 0.0)
        own[g] = block.astype(jnp.bfloat16)


def masked(side, ranks, amplitudes):
    shape = amplitudes.shape
    return pl.pallas_call(
        start_kernel,
        grid_spec=pltpu.PrefetchScalarGridSpec(
            num_scalar_prefetch=2,
            grid=(1,),
            in_specs=[pl.BlockSpec(shape, lambda i, *_: (0, 0, 0))],
            out_specs=pl.BlockSpec(shape, lambda i, *_: (0, 0, 0)),
        ),
        out_shape=jax.ShapeDtypeStruct(shape, jnp.bfloat16),
        compiler_params=pltpu.CompilerParams(vmem_limit_bytes=8 * 1024 * 1024),
        name="masked",
    )(side, ranks, amplitudes)


def arrange_kernel(side, after, over, across, halves):
    terms, width = over.shape[1], over.shape[2]
    half = width // 2
    row = lax.broadcasted_iota(jnp.int32, (width, width), 0)
    lane = lax.broadcasted_iota(jnp.int32, (width, width), 1)
    first = side[0] * half
    even = ((lane < half) & (row == lane + first)).astype(jnp.bfloat16)
    odd = ((lane >= half) & (row == lane - half + first)).astype(jnp.bfloat16)
    picks = jnp.concatenate([even, odd], axis=0)
    for n in range(0, terms, 2):
        two = jnp.concatenate([over[0, n], over[0, n + 1]], axis=1)
        picked = jnp.dot(two, picks, preferred_element_type=jnp.float32).astype(jnp.bfloat16)
        halves[0, :, n * half : (n + 2) * half] = picked
    for n in range(terms):
        across[0, n] = over[0, n].T


def arrange(side, after, over):
    count, terms, width, _ = over.shape
    across = (count, terms, width, width)
    halves = (count, width, terms * width // 2)
    return pl.pallas_call(
        arrange_kernel,
        grid_spec=pltpu.PrefetchScalarGridSpec(
            num_scalar_prefetch=1,
            grid=(count,),
            in_specs=[
                pl.BlockSpec((1, *after.shape[1:]), lambda g, *_: (0, 0, 0)),
                pl.BlockSpec((1, *over.shape[1:]), lambda g, *_: (g, 0, 0, 0)),
            ],
            out_specs=[
                pl.BlockSpec((1, *across[1:]), lambda g, *_: (g, 0, 0, 0)),
                pl.BlockSpec((1, *halves[1:]), lambda g, *_: (g, 0, 0)),
            ],
        ),
        out_shape=(
            pltpu.VMEM(across, over.dtype),
            pltpu.VMEM(halves, over.dtype),
        ),
        compiler_params=pltpu.CompilerParams(
            dimension_semantics=("arbitrary",), vmem_limit_bytes=24 * 1024 * 1024
        ),
        cost_estimate=pl.CostEstimate(flops=10**9, transcendentals=0, bytes_accessed=3 * over.size),
        name="arrange",
    )(side, after, over)


def couple_kernel(side, slots, weights, across, halves, *refs):
    pieces, (mine, theirs, window, stacks) = refs[:-4], refs[-4:]
    count, terms, width, _ = across.shape
    size, half, _ = pieces[0].shape
    for place, piece in enumerate(pieces):
        window[place * size : (place + 1) * size] = piece[...]

    def right_side(g, stack):
        for n in range(terms):
            place = g * terms + n
            right = jnp.dot(
                window[slots[place]], across[g, n], preferred_element_type=jnp.float32
            )
            stack[n * half : (n + 1) * half] = (right * weights[place]).astype(jnp.bfloat16)

    def left_side(g, stack):
        both = jnp.dot(halves[g], stack[...], preferred_element_type=jnp.float32)
        upper = side[0] == 0
        mine[g] = jnp.where(upper, both[:half], both[half:])
        theirs[g] = jnp.where(upper, both[half:], both[:half])

    right_side(0, stacks.at[0])

    def step(g, carry):
        right_side(g, stacks.at[lax.rem(g, 2)])
        left_side(g - 1, stacks.at[lax.rem(g - 1, 2)])
        return carry

    lax.fori_loop(1, count, step, 0)
    left_side(count - 1, stacks.at[(count - 1) % 2])


def couple(side, slots, weights, across, halves, pieces):
    count, terms, width, _ = across.shape
    size, half, _ = pieces[0].shape
    inside = pl.BlockSpec(memory_space=pltpu.VMEM)
    scalars = pl.BlockSpec(memory_space=pltpu.SMEM)
    return pl.pallas_call(
        couple_kernel,
        in_specs=[scalars] * 3 + [inside] * (2 + len(pieces)),
        out_specs=[inside] * 2,
        out_shape=[jax.ShapeDtypeStruct((count, half, width), jnp.float32)] * 2,
        scratch_shapes=[
            pltpu.VMEM((len(pieces) * size, half, width), jnp.bfloat16),
            pltpu.VMEM((2, terms * half, width), jnp.bfloat16),
        ],
        compiler_params=pltpu.CompilerParams(vmem_limit_bytes=24 * 1024 * 1024),
        name="couple",
    )(side, slots, weights, across, halves, *pieces)


def products_kernel(scale, mine, theirs, mask, *refs):
    held, (last, sums) = refs[:-2], refs[-2:]
    last[...] = mask[...] * (mine[...] + theirs[...]) - held[-1][...]
    terms = [ref[...] * scale for ref in held] + [last[...] * scale]
    lane = lax.broadcasted_iota(jnp.int32, sums.shape, 1)
    row = jnp.zeros(sums.shape, jnp.float32)
    for place, (i, j) in enumerate(PRODUCTS):
        row = jnp.where(lane == place, jnp.sum(terms[i] * terms[j]), row)
    sums[...] = row


def products(scale, mine, theirs, mask, held):
    shape = mask.shape
    inside = pl.BlockSpec(memory_space=pltpu.VMEM)
    return pl.pallas_call(
        lambda *refs: products_kernel(scale, *refs),
        in_specs=[inside] * (3 + len(held)),
        out_specs=(inside, inside),
        out_shape=(
            jax.ShapeDtypeStruct(shape, jnp.float32),
            jax.ShapeDtypeStruct((1, shape[-1]), jnp.float32),
        ),
        compiler_params=pltpu.CompilerParams(vmem_limit_bytes=8 * 1024 * 1024),
        name="products",
    )(mine, theirs, mask, *held)


def finish_kernel(copies, own, denom, *refs):
    terms, (amps, norms) = refs[:-2], refs[-2:]
    total = jnp.sum(copies[...], axis=0)
    gram = {}
    for place, (i, j) in enumerate(PRODUCTS):
        gram[i, j] = gram[j, i] = total[:, place : place + 1]
    one = jnp.ones_like(gram[0, 0])
    shares = [one] + [jnp.zeros_like(one)] * (ITERS - 1)
    sums = [jnp.zeros_like(one)] * ITERS
    for step_no in range(ITERS):
        square = jnp.zeros_like(one)
        for i in range(step_no + 1):
            for j in range(step_no + 1):
                square = square + (shares[i] * gram[i, j]) * shares[j]
        rms = jnp.sqrt(jnp.maximum(square, 0.0))
        norms[step_no] = rms[0, 0]
        factor = 1.0 / (1.0 + rms)
        sums = [held + factor * share for held, share in zip(sums, shares, strict=True)]
        shares = [shares[0]] + [
            shares[i] + factor * shares[i - 1] for i in range(1, ITERS)
        ]
    change = sum(held * ref[...].reshape(-1, own.shape[-1]) for held, ref in zip(sums, terms, strict=True))
    change = change.reshape(own.shape)
    amps[...] = (own[...].astype(jnp.float32) + change / denom[...]).astype(jnp.bfloat16)


def finish(copies, own, denom, terms):
    return pl.pallas_call(
        finish_kernel,
        out_shape=(
            jax.ShapeDtypeStruct(own.shape, jnp.bfloat16),
            jax.ShapeDtypeStruct((ITERS,), jnp.float32),
        ),
        in_specs=[pl.BlockSpec(memory_space=pltpu.VMEM)] * (3 + len(terms)),
        out_specs=(pl.BlockSpec(memory_space=pltpu.VMEM), pl.BlockSpec(memory_space=pltpu.SMEM)),
        compiler_params=pltpu.CompilerParams(vmem_limit_bytes=8 * 1024 * 1024),
        name="finish",
    )(copies, own, denom, *terms)


def per_device(
    amplitudes, integrals, intersections, coupling, pno_energies, pair_shift, ranks, neighbours
):
    count, half, width = amplitudes.shape
    chain_pos = lax.axis_index("chain")
    side = lax.axis_index("pno")
    first_row = side * half
    frag = count * lax.axis_size("pair")
    cells = frag * lax.axis_size("chain") * width * width
    sides = jnp.reshape(side, (1,)).astype(jnp.int32)
    own = masked(sides, ranks, amplitudes)
    columns = jnp.arange(width, dtype=jnp.int32)
    rows_here = first_row + jnp.arange(half, dtype=jnp.int32)
    live_cols = columns[None, :] < ranks[:, None]
    live_rows = rows_here[None, :] < ranks[:, None]
    mask = (live_rows[:, :, None] & live_cols[:, None, :]).astype(jnp.float32)
    energy_rows = lax.dynamic_slice_in_dim(pno_energies, first_row, half, 1)
    denom = energy_rows[:, :, None] + pno_energies[:, None, :] - pair_shift[:, None, None]
    within = neighbours % frag
    place = within // count
    turn = (place - lax.axis_index("pair")) % 2
    piece_no = 2 * (neighbours // frag - chain_pos + 1) + turn
    near = lax.axis_size("pair") // 2
    slots = ((piece_no * near + place // 2) * count + within % count).reshape(-1)
    weights = coupling.reshape(-1)
    over = pltpu.with_memory_space_constraint(intersections, pltpu.HBM)

    kept = []

    def coupled_parts(piece):
        pieces = spread(piece)
        if not kept:
            kept.extend(arrange(sides, pieces[2], over))
        mine, theirs = couple(sides, slots, weights, *kept, pieces)
        return mine, shifted(theirs, "pno", 1, around=True)

    mine, theirs = coupled_parts(own)
    ints = integrals.astype(jnp.float32)
    terms = [mask * (ints + (mine + theirs) - denom * own.astype(jnp.float32))]
    for step_no in range(1, ITERS):
        mine, theirs = coupled_parts((terms[-1] / denom).astype(jnp.bfloat16))
        if step_no + 1 < ITERS:
            terms.append(mask * (mine + theirs) - terms[-1])
    last, sums = products(cells**-0.5, mine, theirs, mask, terms)
    sums = sums + shifted(sums, "pno", 1, around=True)
    rest = ("chain", "pair")
    sums = jnp.broadcast_to(sums, (lax.axis_size(rest), *sums.shape))
    return tuple(finish(lax.all_to_all(sums, rest, 0, 0, tiled=True), own, denom, terms + [last]))


def solution(mesh):
    in_specs = (
        P(("job", "chain", "pair"), "pno", None),
        P(("job", "chain", "pair"), "pno", None),
        P(("job", "chain", "pair"), None, None, None),
        P(("job", "chain", "pair"), None),
        P(("job", "chain", "pair"), None),
        P(("job", "chain", "pair")),
        P(("job", "chain", "pair")),
        P(("job", "chain", "pair"), None),
    )
    out_specs = (P(("job", "chain", "pair"), "pno", None), P("job"))
    return jax.shard_map(
        per_device, mesh=mesh, in_specs=in_specs, out_specs=out_specs, check_vma=False
    )
```

```python
import jax
import jax.numpy as jnp
from jax import lax
from jax.experimental import pallas as pl
from jax.experimental.pallas import tpu as pltpu
from jax.sharding import PartitionSpec as P

ITERS = 3
PRODUCTS = [(i, j) for i in range(ITERS) for j in range(i + 1)]


def shifted(value, axis, step, around=False):
    count = lax.axis_size(axis)
    pairs = [(i, (i + step) % count) for i in range(count) if around or 0 <= i + step < count]
    return lax.ppermute(value, axis, pairs)


def spread(piece):
    count = lax.axis_size("pair")
    groups = [list(range(first, count, 2)) for first in range(2)]
    copies = jnp.broadcast_to(piece, (len(groups[0]), *piece.shape))
    near = lax.all_to_all(copies, "pair", 0, 0, tiled=True, axis_index_groups=groups)
    near = near.reshape(-1, *piece.shape[1:])
    low, high = shifted(near, "chain", 1), shifted(near, "chain", -1)
    other = shifted(near, "pair", 1, around=True)
    low_other = shifted(low, "pair", 1, around=True)
    high_other = shifted(high, "pair", -1, around=True)
    return low, low_other, near, other, high, high_other


def live_cells(rank, first, half, width):
    rows = first + lax.broadcasted_iota(jnp.int32, (half, width), 0)
    columns = lax.broadcasted_iota(jnp.int32, (half, width), 1)
    return (rows < rank) & (columns < rank)


def start_kernel(side, ranks, amplitudes, own):
    count, half, width = amplitudes.shape
    for g in range(count):
        live = live_cells(ranks[g], side[0] * half, half, width)
        block = jnp.where(live, amplitudes[g].astype(jnp.float32), 0.0)
        own[g] = block.astype(jnp.bfloat16)


def masked(side, ranks, amplitudes):
    shape = amplitudes.shape
    return pl.pallas_call(
        start_kernel,
        grid_spec=pltpu.PrefetchScalarGridSpec(
            num_scalar_prefetch=2,
            grid=(1,),
            in_specs=[pl.BlockSpec(shape, lambda i, *_: (0, 0, 0))],
            out_specs=pl.BlockSpec(shape, lambda i, *_: (0, 0, 0)),
        ),
        out_shape=jax.ShapeDtypeStruct(shape, jnp.bfloat16),
        compiler_params=pltpu.CompilerParams(vmem_limit_bytes=8 * 1024 * 1024),
        name="masked",
    )(side, ranks, amplitudes)


def arrange_kernel(side, after, over, across, halves):
    terms, width = over.shape[1], over.shape[2]
    half = width // 2
    row = lax.broadcasted_iota(jnp.int32, (width, width), 0)
    lane = lax.broadcasted_iota(jnp.int32, (width, width), 1)
    first = side[0] * half
    even = ((lane < half) & (row == lane + first)).astype(jnp.bfloat16)
    odd = ((lane >= half) & (row == lane - half + first)).astype(jnp.bfloat16)
    picks = jnp.concatenate([even, odd], axis=0)
    for n in range(0, terms, 2):
        two = jnp.concatenate([over[0, n], over[0, n + 1]], axis=1)
        picked = jnp.dot(two, picks, preferred_element_type=jnp.float32).astype(jnp.bfloat16)
        halves[0, :, n * half : (n + 2) * half] = picked
    for n in range(terms):
        across[0, n] = over[0, n].T


def arrange(side, after, over):
    count, terms, width, _ = over.shape
    across = (count, terms, width, width)
    halves = (count, width, terms * width // 2)
    return pl.pallas_call(
        arrange_kernel,
        grid_spec=pltpu.PrefetchScalarGridSpec(
            num_scalar_prefetch=1,
            grid=(count,),
            in_specs=[
                pl.BlockSpec((1, *after.shape[1:]), lambda g, *_: (0, 0, 0)),
                pl.BlockSpec((1, *over.shape[1:]), lambda g, *_: (g, 0, 0, 0)),
            ],
            out_specs=[
                pl.BlockSpec((1, *across[1:]), lambda g, *_: (g, 0, 0, 0)),
                pl.BlockSpec((1, *halves[1:]), lambda g, *_: (g, 0, 0)),
            ],
        ),
        out_shape=(
            pltpu.VMEM(across, over.dtype),
            pltpu.VMEM(halves, over.dtype),
        ),
        compiler_params=pltpu.CompilerParams(
            dimension_semantics=("arbitrary",), vmem_limit_bytes=24 * 1024 * 1024
        ),
        cost_estimate=pl.CostEstimate(flops=10**9, transcendentals=0, bytes_accessed=3 * over.size),
        name="arrange",
    )(side, after, over)


def couple_kernel(side, slots, weights, across, halves, *refs):
    pieces, (mine, theirs, window, stacks) = refs[:-4], refs[-4:]
    count, terms, width, _ = across.shape
    size, half, _ = pieces[0].shape
    for place, piece in enumerate(pieces):
        window[place * size : (place + 1) * size] = piece[...]

    def right_side(g, stack):
        for n in range(terms):
            place = g * terms + n
            right = jnp.dot(
                window[slots[place]], across[g, n], preferred_element_type=jnp.float32
            )
            stack[n * half : (n + 1) * half] = (right * weights[place]).astype(jnp.bfloat16)

    def left_side(g, stack):
        both = jnp.dot(halves[g], stack[...], preferred_element_type=jnp.float32)
        upper = side[0] == 0
        mine[g] = jnp.where(upper, both[:half], both[half:])
        theirs[g] = jnp.where(upper, both[half:], both[:half])

    right_side(0, stacks.at[0])

    def step(g, carry):
        right_side(g, stacks.at[lax.rem(g, 2)])
        left_side(g - 1, stacks.at[lax.rem(g - 1, 2)])
        return carry

    lax.fori_loop(1, count, step, 0)
    left_side(count - 1, stacks.at[(count - 1) % 2])


def couple(side, slots, weights, across, halves, pieces):
    count, terms, width, _ = across.shape
    size, half, _ = pieces[0].shape
    inside = pl.BlockSpec(memory_space=pltpu.VMEM)
    scalars = pl.BlockSpec(memory_space=pltpu.SMEM)
    return pl.pallas_call(
        couple_kernel,
        in_specs=[scalars] * 3 + [inside] * (2 + len(pieces)),
        out_specs=[inside] * 2,
        out_shape=[jax.ShapeDtypeStruct((count, half, width), jnp.float32)] * 2,
        scratch_shapes=[
            pltpu.VMEM((len(pieces) * size, half, width), jnp.bfloat16),
            pltpu.VMEM((2, terms * half, width), jnp.bfloat16),
        ],
        compiler_params=pltpu.CompilerParams(vmem_limit_bytes=24 * 1024 * 1024),
        name="couple",
    )(side, slots, weights, across, halves, *pieces)


def products_kernel(scale, mine, theirs, mask, *refs):
    held, (last, sums) = refs[:-2], refs[-2:]
    last[...] = mask[...] * (mine[...] + theirs[...]) - held[-1][...]
    terms = [ref[...] * scale for ref in held] + [last[...] * scale]
    lane = lax.broadcasted_iota(jnp.int32, sums.shape, 2)
    row = jnp.zeros(sums.shape, jnp.float32)
    for place, (i, j) in enumerate(PRODUCTS):
        row = jnp.where(lane == place, jnp.sum(terms[i] * terms[j]), row)
    sums[...] = row


def products(scale, mine, theirs, mask, held, count):
    shape = mask.shape
    inside = pl.BlockSpec(memory_space=pltpu.VMEM)
    return pl.pallas_call(
        lambda *refs: products_kernel(scale, *refs),
        in_specs=[inside] * (3 + len(held)),
        out_specs=(inside, inside),
        out_shape=(
            jax.ShapeDtypeStruct(shape, jnp.float32),
            jax.ShapeDtypeStruct((count, 1, shape[-1]), jnp.float32),
        ),
        compiler_params=pltpu.CompilerParams(vmem_limit_bytes=8 * 1024 * 1024),
        name="products",
    )(mine, theirs, mask, *held)


def finish_kernel(copies, own, denom, *refs):
    terms, (amps, norms) = refs[:-2], refs[-2:]
    total = jnp.sum(copies[...], axis=0)
    gram = {}
    for place, (i, j) in enumerate(PRODUCTS):
        gram[i, j] = gram[j, i] = total[:, place : place + 1]
    one = jnp.ones_like(gram[0, 0])
    shares = [one] + [jnp.zeros_like(one)] * (ITERS - 1)
    sums = [jnp.zeros_like(one)] * ITERS
    for step_no in range(ITERS):
        square = jnp.zeros_like(one)
        for i in range(step_no + 1):
            for j in range(step_no + 1):
                square = square + (shares[i] * gram[i, j]) * shares[j]
        rms = jnp.sqrt(jnp.maximum(square, 0.0))
        norms[step_no] = rms[0, 0]
        factor = 1.0 / (1.0 + rms)
        sums = [held + factor * share for held, share in zip(sums, shares, strict=True)]
        shares = [shares[0]] + [
            shares[i] + factor * shares[i - 1] for i in range(1, ITERS)
        ]
    change = sum(held * ref[...].reshape(-1, own.shape[-1]) for held, ref in zip(sums, terms, strict=True))
    change = change.reshape(own.shape)
    amps[...] = (own[...].astype(jnp.float32) + change / denom[...]).astype(jnp.bfloat16)


def finish(copies, own, denom, terms):
    return pl.pallas_call(
        finish_kernel,
        out_shape=(
            jax.ShapeDtypeStruct(own.shape, jnp.bfloat16),
            jax.ShapeDtypeStruct((ITERS,), jnp.float32),
        ),
        in_specs=[pl.BlockSpec(memory_space=pltpu.VMEM)] * (3 + len(terms)),
        out_specs=(pl.BlockSpec(memory_space=pltpu.VMEM), pl.BlockSpec(memory_space=pltpu.SMEM)),
        compiler_params=pltpu.CompilerParams(vmem_limit_bytes=8 * 1024 * 1024),
        name="finish",
    )(copies, own, denom, *terms)


def per_device(
    amplitudes, integrals, intersections, coupling, pno_energies, pair_shift, ranks, neighbours
):
    count, half, width = amplitudes.shape
    chain_pos = lax.axis_index("chain")
    side = lax.axis_index("pno")
    first_row = side * half
    frag = count * lax.axis_size("pair")
    cells = frag * lax.axis_size("chain") * width * width
    sides = jnp.reshape(side, (1,)).astype(jnp.int32)
    own = masked(sides, ranks, amplitudes)
    columns = jnp.arange(width, dtype=jnp.int32)
    rows_here = first_row + jnp.arange(half, dtype=jnp.int32)
    live_cols = columns[None, :] < ranks[:, None]
    live_rows = rows_here[None, :] < ranks[:, None]
    mask = (live_rows[:, :, None] & live_cols[:, None, :]).astype(jnp.float32)
    energy_rows = lax.dynamic_slice_in_dim(pno_energies, first_row, half, 1)
    denom = energy_rows[:, :, None] + pno_energies[:, None, :] - pair_shift[:, None, None]
    within = neighbours % frag
    place = within // count
    turn = (place - lax.axis_index("pair")) % 2
    piece_no = 2 * (neighbours // frag - chain_pos + 1) + turn
    near = lax.axis_size("pair") // 2
    slots = ((piece_no * near + place // 2) * count + within % count).reshape(-1)
    weights = coupling.reshape(-1)
    over = pltpu.with_memory_space_constraint(intersections, pltpu.HBM)

    kept = []

    def coupled_parts(piece):
        pieces = spread(piece)
        if not kept:
            kept.extend(arrange(sides, pieces[2], over))
        mine, theirs = couple(sides, slots, weights, *kept, pieces)
        return mine, shifted(theirs, "pno", 1, around=True)

    mine, theirs = coupled_parts(own)
    ints = integrals.astype(jnp.float32)
    terms = [mask * (ints + (mine + theirs) - denom * own.astype(jnp.float32))]
    for step_no in range(1, ITERS):
        mine, theirs = coupled_parts((terms[-1] / denom).astype(jnp.bfloat16))
        if step_no + 1 < ITERS:
            terms.append(mask * (mine + theirs) - terms[-1])
    lines = lax.axis_size("chain") * lax.axis_size("pno")
    last, sums = products(cells**-0.5, mine, theirs, mask, terms, lines)
    sums = lax.all_to_all(sums, ("chain", "pno"), 0, 0, tiled=True)
    sums = jnp.broadcast_to(jnp.sum(sums, axis=0), (lax.axis_size("pair"), 1, width))
    sums = lax.all_to_all(sums, "pair", 0, 0, tiled=True)
    return tuple(finish(sums, own, denom, terms + [last]))


def solution(mesh):
    in_specs = (
        P(("job", "chain", "pair"), "pno", None),
        P(("job", "chain", "pair"), "pno", None),
        P(("job", "chain", "pair"), None, None, None),
        P(("job", "chain", "pair"), None),
        P(("job", "chain", "pair"), None),
        P(("job", "chain", "pair")),
        P(("job", "chain", "pair")),
        P(("job", "chain", "pair"), None),
    )
    out_specs = (P(("job", "chain", "pair"), "pno", None), P("job"))
    return jax.shard_map(
        per_device, mesh=mesh, in_specs=in_specs, out_specs=out_specs, check_vma=False
    )
```

```python
import jax
import jax.numpy as jnp
from jax import lax
from jax.experimental import pallas as pl
from jax.experimental.pallas import tpu as pltpu
from jax.sharding import PartitionSpec as P

ITERS = 3
PRODUCTS = [(i, j) for i in range(ITERS) for j in range(i + 1)]


def shifted(value, axis, step, around=False):
    count = lax.axis_size(axis)
    pairs = [(i, (i + step) % count) for i in range(count) if around or 0 <= i + step < count]
    return lax.ppermute(value, axis, pairs)


def crossed(value, axis, step, around):
    count, sides = lax.axis_size(axis), lax.axis_size("pno")
    pairs = []
    for i in range(count):
        for side in range(sides):
            to = i + (step if side % 2 == 0 else -step)
            if around or 0 <= to < count:
                pairs.append((i * sides + side, to % count * sides + side))
    return lax.ppermute(value, (axis, "pno"), pairs)


def spread(piece):
    count = lax.axis_size("pair")
    groups = [list(range(first, count, 2)) for first in range(2)]
    copies = jnp.broadcast_to(piece, (len(groups[0]), *piece.shape))
    near = lax.all_to_all(copies, "pair", 0, 0, tiled=True, axis_index_groups=groups)
    near = near.reshape(-1, *piece.shape[1:])
    fore, back = crossed(near, "chain", 1, False), crossed(near, "chain", -1, False)
    other = crossed(near, "pair", 1, True)
    fore_other = crossed(fore, "pair", 1, True)
    back_other = crossed(back, "pair", -1, True)
    return fore, fore_other, near, other, back, back_other


def live_cells(rank, first, half, width):
    rows = first + lax.broadcasted_iota(jnp.int32, (half, width), 0)
    columns = lax.broadcasted_iota(jnp.int32, (half, width), 1)
    return (rows < rank) & (columns < rank)


def start_kernel(side, ranks, amplitudes, own):
    count, half, width = amplitudes.shape
    for g in range(count):
        live = live_cells(ranks[g], side[0] * half, half, width)
        block = jnp.where(live, amplitudes[g].astype(jnp.float32), 0.0)
        own[g] = block.astype(jnp.bfloat16)


def masked(side, ranks, amplitudes):
    shape = amplitudes.shape
    return pl.pallas_call(
        start_kernel,
        grid_spec=pltpu.PrefetchScalarGridSpec(
            num_scalar_prefetch=2,
            grid=(1,),
            in_specs=[pl.BlockSpec(shape, lambda i, *_: (0, 0, 0))],
            out_specs=pl.BlockSpec(shape, lambda i, *_: (0, 0, 0)),
        ),
        out_shape=jax.ShapeDtypeStruct(shape, jnp.bfloat16),
        compiler_params=pltpu.CompilerParams(vmem_limit_bytes=8 * 1024 * 1024),
        name="masked",
    )(side, ranks, amplitudes)


def arrange_kernel(side, after, over, across, halves):
    terms, width = over.shape[1], over.shape[2]
    half = width // 2
    row = lax.broadcasted_iota(jnp.int32, (width, width), 0)
    lane = lax.broadcasted_iota(jnp.int32, (width, width), 1)
    first = side[0] * half
    even = ((lane < half) & (row == lane + first)).astype(jnp.bfloat16)
    odd = ((lane >= half) & (row == lane - half + first)).astype(jnp.bfloat16)
    picks = jnp.concatenate([even, odd], axis=0)
    for n in range(0, terms, 2):
        two = jnp.concatenate([over[0, n], over[0, n + 1]], axis=1)
        picked = jnp.dot(two, picks, preferred_element_type=jnp.float32).astype(jnp.bfloat16)
        halves[0, :, n * half : (n + 2) * half] = picked
    for n in range(terms):
        across[0, n] = over[0, n].T


def arrange(side, after, over):
    count, terms, width, _ = over.shape
    across = (count, terms, width, width)
    halves = (count, width, terms * width // 2)
    return pl.pallas_call(
        arrange_kernel,
        grid_spec=pltpu.PrefetchScalarGridSpec(
            num_scalar_prefetch=1,
            grid=(count,),
            in_specs=[
                pl.BlockSpec((1, *after.shape[1:]), lambda g, *_: (0, 0, 0)),
                pl.BlockSpec((1, *over.shape[1:]), lambda g, *_: (g, 0, 0, 0)),
            ],
            out_specs=[
                pl.BlockSpec((1, *across[1:]), lambda g, *_: (g, 0, 0, 0)),
                pl.BlockSpec((1, *halves[1:]), lambda g, *_: (g, 0, 0)),
            ],
        ),
        out_shape=(
            pltpu.VMEM(across, over.dtype),
            pltpu.VMEM(halves, over.dtype),
        ),
        compiler_params=pltpu.CompilerParams(
            dimension_semantics=("arbitrary",), vmem_limit_bytes=24 * 1024 * 1024
        ),
        cost_estimate=pl.CostEstimate(flops=10**9, transcendentals=0, bytes_accessed=3 * over.size),
        name="arrange",
    )(side, after, over)


def couple_kernel(side, slots, weights, across, halves, *refs):
    pieces, (mine, theirs, window, stacks) = refs[:-4], refs[-4:]
    count, terms, width, _ = across.shape
    size, half, _ = pieces[0].shape
    for place, piece in enumerate(pieces):
        window[place * size : (place + 1) * size] = piece[...]

    def right_side(g, stack):
        for n in range(terms):
            place = g * terms + n
            right = jnp.dot(
                window[slots[place]], across[g, n], preferred_element_type=jnp.float32
            )
            stack[n * half : (n + 1) * half] = (right * weights[place]).astype(jnp.bfloat16)

    def left_side(g, stack):
        both = jnp.dot(halves[g], stack[...], preferred_element_type=jnp.float32)
        upper = side[0] == 0
        mine[g] = jnp.where(upper, both[:half], both[half:])
        theirs[g] = jnp.where(upper, both[half:], both[:half])

    right_side(0, stacks.at[0])

    def step(g, carry):
        left_side(g - 1, stacks.at[lax.rem(g - 1, 2)])
        right_side(g, stacks.at[lax.rem(g, 2)])
        return carry

    lax.fori_loop(1, count, step, 0)
    left_side(count - 1, stacks.at[(count - 1) % 2])


def couple(side, slots, weights, across, halves, pieces):
    count, terms, width, _ = across.shape
    size, half, _ = pieces[0].shape
    inside = pl.BlockSpec(memory_space=pltpu.VMEM)
    scalars = pl.BlockSpec(memory_space=pltpu.SMEM)
    return pl.pallas_call(
        couple_kernel,
        in_specs=[scalars] * 3 + [inside] * (2 + len(pieces)),
        out_specs=[inside] * 2,
        out_shape=[jax.ShapeDtypeStruct((count, half, width), jnp.float32)] * 2,
        scratch_shapes=[
            pltpu.VMEM((len(pieces) * size, half, width), jnp.bfloat16),
            pltpu.VMEM((2, terms * half, width), jnp.bfloat16),
        ],
        compiler_params=pltpu.CompilerParams(vmem_limit_bytes=24 * 1024 * 1024),
        name="couple",
    )(side, slots, weights, across, halves, *pieces)


def products_kernel(scale, mine, theirs, mask, *refs):
    held, (last, sums) = refs[:-2], refs[-2:]
    last[...] = mask[...] * (mine[...] + theirs[...]) - held[-1][...]
    terms = [ref[...] * scale for ref in held] + [last[...] * scale]
    lane = lax.broadcasted_iota(jnp.int32, sums.shape, 2)
    row = jnp.zeros(sums.shape, jnp.float32)
    for place, (i, j) in enumerate(PRODUCTS):
        row = jnp.where(lane == place, jnp.sum(terms[i] * terms[j]), row)
    sums[...] = row


def products(scale, mine, theirs, mask, held, count):
    shape = mask.shape
    inside = pl.BlockSpec(memory_space=pltpu.VMEM)
    return pl.pallas_call(
        lambda *refs: products_kernel(scale, *refs),
        in_specs=[inside] * (3 + len(held)),
        out_specs=(inside, inside),
        out_shape=(
            jax.ShapeDtypeStruct(shape, jnp.float32),
            jax.ShapeDtypeStruct((count, 1, shape[-1]), jnp.float32),
        ),
        compiler_params=pltpu.CompilerParams(vmem_limit_bytes=8 * 1024 * 1024),
        name="products",
    )(mine, theirs, mask, *held)


def finish_kernel(copies, own, denom, *refs):
    terms, (amps, norms) = refs[:-2], refs[-2:]
    total = jnp.sum(copies[...], axis=0)
    gram = {}
    for place, (i, j) in enumerate(PRODUCTS):
        gram[i, j] = gram[j, i] = total[:, place : place + 1]
    one = jnp.ones_like(gram[0, 0])
    shares = [one] + [jnp.zeros_like(one)] * (ITERS - 1)
    sums = [jnp.zeros_like(one)] * ITERS
    for step_no in range(ITERS):
        square = jnp.zeros_like(one)
        for i in range(step_no + 1):
            for j in range(step_no + 1):
                square = square + (shares[i] * gram[i, j]) * shares[j]
        rms = jnp.sqrt(jnp.maximum(square, 0.0))
        norms[step_no] = rms[0, 0]
        factor = 1.0 / (1.0 + rms)
        sums = [held + factor * share for held, share in zip(sums, shares, strict=True)]
        shares = [shares[0]] + [
            shares[i] + factor * shares[i - 1] for i in range(1, ITERS)
        ]
    change = sum(held * ref[...].reshape(-1, own.shape[-1]) for held, ref in zip(sums, terms, strict=True))
    change = change.reshape(own.shape)
    amps[...] = (own[...].astype(jnp.float32) + change / denom[...]).astype(jnp.bfloat16)


def finish(copies, own, denom, terms):
    return pl.pallas_call(
        finish_kernel,
        out_shape=(
            jax.ShapeDtypeStruct(own.shape, jnp.bfloat16),
            jax.ShapeDtypeStruct((ITERS,), jnp.float32),
        ),
        in_specs=[pl.BlockSpec(memory_space=pltpu.VMEM)] * (3 + len(terms)),
        out_specs=(pl.BlockSpec(memory_space=pltpu.VMEM), pl.BlockSpec(memory_space=pltpu.SMEM)),
        compiler_params=pltpu.CompilerParams(vmem_limit_bytes=8 * 1024 * 1024),
        name="finish",
    )(copies, own, denom, *terms)


def per_device(
    amplitudes, integrals, intersections, coupling, pno_energies, pair_shift, ranks, neighbours
):
    count, half, width = amplitudes.shape
    chain_pos = lax.axis_index("chain")
    side = lax.axis_index("pno")
    first_row = side * half
    frag = count * lax.axis_size("pair")
    cells = frag * lax.axis_size("chain") * width * width
    sides = jnp.reshape(side, (1,)).astype(jnp.int32)
    own = masked(sides, ranks, amplitudes)
    columns = jnp.arange(width, dtype=jnp.int32)
    rows_here = first_row + jnp.arange(half, dtype=jnp.int32)
    live_cols = columns[None, :] < ranks[:, None]
    live_rows = rows_here[None, :] < ranks[:, None]
    mask = (live_rows[:, :, None] & live_cols[:, None, :]).astype(jnp.float32)
    energy_rows = lax.dynamic_slice_in_dim(pno_energies, first_row, half, 1)
    denom = energy_rows[:, :, None] + pno_energies[:, None, :] - pair_shift[:, None, None]
    within = neighbours % frag
    place = within // count
    turn = (place - lax.axis_index("pair")) % 2
    offset = neighbours // frag - chain_pos
    piece_no = 2 * (jnp.where(side == 0, offset, -offset) + 1) + turn
    near = lax.axis_size("pair") // 2
    slots = ((piece_no * near + place // 2) * count + within % count).reshape(-1)
    weights = coupling.reshape(-1)
    over = pltpu.with_memory_space_constraint(intersections, pltpu.HBM)

    kept = []

    def coupled_parts(piece):
        pieces = spread(piece)
        if not kept:
            kept.extend(arrange(sides, pieces[2], over))
        mine, theirs = couple(sides, slots, weights, *kept, pieces)
        return mine, shifted(theirs, "pno", 1, around=True)

    mine, theirs = coupled_parts(own)
    ints = integrals.astype(jnp.float32)
    terms = [mask * (ints + (mine + theirs) - denom * own.astype(jnp.float32))]
    for step_no in range(1, ITERS):
        mine, theirs = coupled_parts((terms[-1] / denom).astype(jnp.bfloat16))
        if step_no + 1 < ITERS:
            terms.append(mask * (mine + theirs) - terms[-1])
    lines = lax.axis_size("chain") * lax.axis_size("pno")
    last, sums = products(cells**-0.5, mine, theirs, mask, terms, lines)
    sums = lax.all_to_all(sums, ("chain", "pno"), 0, 0, tiled=True)
    sums = jnp.broadcast_to(jnp.sum(sums, axis=0), (lax.axis_size("pair"), 1, width))
    sums = lax.all_to_all(sums, "pair", 0, 0, tiled=True)
    return tuple(finish(sums, own, denom, terms + [last]))


def solution(mesh):
    in_specs = (
        P(("job", "chain", "pair"), "pno", None),
        P(("job", "chain", "pair"), "pno", None),
        P(("job", "chain", "pair"), None, None, None),
        P(("job", "chain", "pair"), None),
        P(("job", "chain", "pair"), None),
        P(("job", "chain", "pair")),
        P(("job", "chain", "pair")),
        P(("job", "chain", "pair"), None),
    )
    out_specs = (P(("job", "chain", "pair"), "pno", None), P("job"))
    return jax.shard_map(
        per_device, mesh=mesh, in_specs=in_specs, out_specs=out_specs, check_vma=False
    )
```

```python
import jax
import jax.numpy as jnp
from jax import lax
from jax.experimental import pallas as pl
from jax.experimental.pallas import tpu as pltpu
from jax.sharding import PartitionSpec as P

ITERS = 3
PRODUCTS = [(i, j) for i in range(ITERS) for j in range(i + 1)]


def shifted(value, axis, step, around=False):
    count = lax.axis_size(axis)
    pairs = [(i, (i + step) % count) for i in range(count) if around or 0 <= i + step < count]
    return lax.ppermute(value, axis, pairs)


def crossed(value, axis, step, around):
    count, sides = lax.axis_size(axis), lax.axis_size("pno")
    pairs = []
    for i in range(count):
        for side in range(sides):
            to = i + (step if side % 2 == 0 else -step)
            if around or 0 <= to < count:
                pairs.append((i * sides + side, to % count * sides + side))
    return lax.ppermute(value, (axis, "pno"), pairs)


def spread(piece):
    count = lax.axis_size("pair")
    groups = [list(range(first, count, 2)) for first in range(2)]
    near = lax.all_gather(piece, "pair", axis=0, tiled=True, axis_index_groups=groups)
    fore, back = crossed(near, "chain", 1, False), crossed(near, "chain", -1, False)
    other = crossed(near, "pair", 1, True)
    fore_other = crossed(fore, "pair", 1, True)
    back_other = crossed(back, "pair", -1, True)
    return fore, fore_other, near, other, back, back_other


def live_cells(rank, first, half, width):
    rows = first + lax.broadcasted_iota(jnp.int32, (half, width), 0)
    columns = lax.broadcasted_iota(jnp.int32, (half, width), 1)
    return (rows < rank) & (columns < rank)


def start_kernel(side, ranks, amplitudes, own):
    count, half, width = amplitudes.shape
    for g in range(count):
        live = live_cells(ranks[g], side[0] * half, half, width)
        block = jnp.where(live, amplitudes[g].astype(jnp.float32), 0.0)
        own[g] = block.astype(jnp.bfloat16)


def masked(side, ranks, amplitudes):
    shape = amplitudes.shape
    return pl.pallas_call(
        start_kernel,
        grid_spec=pltpu.PrefetchScalarGridSpec(
            num_scalar_prefetch=2,
            grid=(1,),
            in_specs=[pl.BlockSpec(shape, lambda i, *_: (0, 0, 0))],
            out_specs=pl.BlockSpec(shape, lambda i, *_: (0, 0, 0)),
        ),
        out_shape=jax.ShapeDtypeStruct(shape, jnp.bfloat16),
        compiler_params=pltpu.CompilerParams(vmem_limit_bytes=8 * 1024 * 1024),
        name="masked",
    )(side, ranks, amplitudes)


def arrange_kernel(side, after, over, across, halves):
    terms, width = over.shape[1], over.shape[2]
    half = width // 2
    row = lax.broadcasted_iota(jnp.int32, (width, width), 0)
    lane = lax.broadcasted_iota(jnp.int32, (width, width), 1)
    first = side[0] * half
    even = ((lane < half) & (row == lane + first)).astype(jnp.bfloat16)
    odd = ((lane >= half) & (row == lane - half + first)).astype(jnp.bfloat16)
    picks = jnp.concatenate([even, odd], axis=0)
    for n in range(0, terms, 2):
        two = jnp.concatenate([over[0, n], over[0, n + 1]], axis=1)
        picked = jnp.dot(two, picks, preferred_element_type=jnp.float32).astype(jnp.bfloat16)
        halves[0, :, n * half : (n + 2) * half] = picked
    for n in range(terms):
        across[0, n] = over[0, n].T


def arrange(side, after, over):
    count, terms, width, _ = over.shape
    across = (count, terms, width, width)
    halves = (count, width, terms * width // 2)
    return pl.pallas_call(
        arrange_kernel,
        grid_spec=pltpu.PrefetchScalarGridSpec(
            num_scalar_prefetch=1,
            grid=(count,),
            in_specs=[
                pl.BlockSpec((1, *after.shape[1:]), lambda g, *_: (0, 0, 0)),
                pl.BlockSpec((1, *over.shape[1:]), lambda g, *_: (g, 0, 0, 0)),
            ],
            out_specs=[
                pl.BlockSpec((1, *across[1:]), lambda g, *_: (g, 0, 0, 0)),
                pl.BlockSpec((1, *halves[1:]), lambda g, *_: (g, 0, 0)),
            ],
        ),
        out_shape=(
            pltpu.VMEM(across, over.dtype),
            pltpu.VMEM(halves, over.dtype),
        ),
        compiler_params=pltpu.CompilerParams(
            dimension_semantics=("arbitrary",), vmem_limit_bytes=24 * 1024 * 1024
        ),
        cost_estimate=pl.CostEstimate(flops=10**9, transcendentals=0, bytes_accessed=3 * over.size),
        name="arrange",
    )(side, after, over)


def couple_kernel(side, slots, weights, across, halves, *refs):
    pieces, (mine, theirs, window, stacks) = refs[:-4], refs[-4:]
    count, terms, width, _ = across.shape
    size, half, _ = pieces[0].shape
    for place, piece in enumerate(pieces):
        window[place * size : (place + 1) * size] = piece[...]

    def right_side(g, stack):
        for n in range(terms):
            place = g * terms + n
            right = jnp.dot(
                window[slots[place]], across[g, n], preferred_element_type=jnp.float32
            )
            stack[n * half : (n + 1) * half] = (right * weights[place]).astype(jnp.bfloat16)

    def left_side(g, stack):
        both = jnp.dot(halves[g], stack[...], preferred_element_type=jnp.float32)
        upper = side[0] == 0
        mine[g] = jnp.where(upper, both[:half], both[half:])
        theirs[g] = jnp.where(upper, both[half:], both[:half])

    right_side(0, stacks.at[0])

    def step(g, carry):
        left_side(g - 1, stacks.at[lax.rem(g - 1, 2)])
        right_side(g, stacks.at[lax.rem(g, 2)])
        return carry

    lax.fori_loop(1, count, step, 0)
    left_side(count - 1, stacks.at[(count - 1) % 2])


def couple(side, slots, weights, across, halves, pieces):
    count, terms, width, _ = across.shape
    size, half, _ = pieces[0].shape
    inside = pl.BlockSpec(memory_space=pltpu.VMEM)
    scalars = pl.BlockSpec(memory_space=pltpu.SMEM)
    return pl.pallas_call(
        couple_kernel,
        in_specs=[scalars] * 3 + [inside] * (2 + len(pieces)),
        out_specs=[inside] * 2,
        out_shape=[jax.ShapeDtypeStruct((count, half, width), jnp.float32)] * 2,
        scratch_shapes=[
            pltpu.VMEM((len(pieces) * size, half, width), jnp.bfloat16),
            pltpu.VMEM((2, terms * half, width), jnp.bfloat16),
        ],
        compiler_params=pltpu.CompilerParams(vmem_limit_bytes=24 * 1024 * 1024),
        name="couple",
    )(side, slots, weights, across, halves, *pieces)


def products_kernel(scale, mine, theirs, mask, *refs):
    held, (last, sums) = refs[:-2], refs[-2:]
    last[...] = mask[...] * (mine[...] + theirs[...]) - held[-1][...]
    terms = [ref[...] * scale for ref in held] + [last[...] * scale]
    lane = lax.broadcasted_iota(jnp.int32, sums.shape, 2)
    row = jnp.zeros(sums.shape, jnp.float32)
    for place, (i, j) in enumerate(PRODUCTS):
        row = jnp.where(lane == place, jnp.sum(terms[i] * terms[j]), row)
    sums[...] = row


def products(scale, mine, theirs, mask, held, count):
    shape = mask.shape
    inside = pl.BlockSpec(memory_space=pltpu.VMEM)
    return pl.pallas_call(
        lambda *refs: products_kernel(scale, *refs),
        in_specs=[inside] * (3 + len(held)),
        out_specs=(inside, inside),
        out_shape=(
            jax.ShapeDtypeStruct(shape, jnp.float32),
            jax.ShapeDtypeStruct((count, 1, shape[-1]), jnp.float32),
        ),
        compiler_params=pltpu.CompilerParams(vmem_limit_bytes=8 * 1024 * 1024),
        name="products",
    )(mine, theirs, mask, *held)


def finish_kernel(copies, own, denom, *refs):
    terms, (amps, norms) = refs[:-2], refs[-2:]
    total = jnp.sum(copies[...], axis=0)
    gram = {}
    for place, (i, j) in enumerate(PRODUCTS):
        gram[i, j] = gram[j, i] = total[:, place : place + 1]
    one = jnp.ones_like(gram[0, 0])
    shares = [one] + [jnp.zeros_like(one)] * (ITERS - 1)
    sums = [jnp.zeros_like(one)] * ITERS
    for step_no in range(ITERS):
        square = jnp.zeros_like(one)
        for i in range(step_no + 1):
            for j in range(step_no + 1):
                square = square + (shares[i] * gram[i, j]) * shares[j]
        rms = jnp.sqrt(jnp.maximum(square, 0.0))
        norms[step_no] = rms[0, 0]
        factor = 1.0 / (1.0 + rms)
        sums = [held + factor * share for held, share in zip(sums, shares, strict=True)]
        shares = [shares[0]] + [
            shares[i] + factor * shares[i - 1] for i in range(1, ITERS)
        ]
    change = sum(held * ref[...].reshape(-1, own.shape[-1]) for held, ref in zip(sums, terms, strict=True))
    change = change.reshape(own.shape)
    amps[...] = (own[...].astype(jnp.float32) + change / denom[...]).astype(jnp.bfloat16)


def finish(copies, own, denom, terms):
    return pl.pallas_call(
        finish_kernel,
        out_shape=(
            jax.ShapeDtypeStruct(own.shape, jnp.bfloat16),
            jax.ShapeDtypeStruct((ITERS,), jnp.float32),
        ),
        in_specs=[pl.BlockSpec(memory_space=pltpu.VMEM)] * (3 + len(terms)),
        out_specs=(pl.BlockSpec(memory_space=pltpu.VMEM), pl.BlockSpec(memory_space=pltpu.SMEM)),
        compiler_params=pltpu.CompilerParams(vmem_limit_bytes=8 * 1024 * 1024),
        name="finish",
    )(copies, own, denom, *terms)


def per_device(
    amplitudes, integrals, intersections, coupling, pno_energies, pair_shift, ranks, neighbours
):
    count, half, width = amplitudes.shape
    chain_pos = lax.axis_index("chain")
    side = lax.axis_index("pno")
    first_row = side * half
    frag = count * lax.axis_size("pair")
    cells = frag * lax.axis_size("chain") * width * width
    sides = jnp.reshape(side, (1,)).astype(jnp.int32)
    own = masked(sides, ranks, amplitudes)
    columns = jnp.arange(width, dtype=jnp.int32)
    rows_here = first_row + jnp.arange(half, dtype=jnp.int32)
    live_cols = columns[None, :] < ranks[:, None]
    live_rows = rows_here[None, :] < ranks[:, None]
    mask = (live_rows[:, :, None] & live_cols[:, None, :]).astype(jnp.float32)
    energy_rows = lax.dynamic_slice_in_dim(pno_energies, first_row, half, 1)
    denom = energy_rows[:, :, None] + pno_energies[:, None, :] - pair_shift[:, None, None]
    within = neighbours % frag
    place = within // count
    turn = (place - lax.axis_index("pair")) % 2
    offset = neighbours // frag - chain_pos
    piece_no = 2 * (jnp.where(side == 0, offset, -offset) + 1) + turn
    near = lax.axis_size("pair") // 2
    slots = ((piece_no * near + place // 2) * count + within % count).reshape(-1)
    weights = coupling.reshape(-1)
    over = pltpu.with_memory_space_constraint(intersections, pltpu.HBM)

    kept = []

    def coupled_parts(piece):
        pieces = spread(piece)
        if not kept:
            kept.extend(arrange(sides, pieces[2], over))
        mine, theirs = couple(sides, slots, weights, *kept, pieces)
        return mine, shifted(theirs, "pno", 1, around=True)

    mine, theirs = coupled_parts(own)
    ints = integrals.astype(jnp.float32)
    terms = [mask * (ints + (mine + theirs) - denom * own.astype(jnp.float32))]
    for step_no in range(1, ITERS):
        mine, theirs = coupled_parts((terms[-1] / denom).astype(jnp.bfloat16))
        if step_no + 1 < ITERS:
            terms.append(mask * (mine + theirs) - terms[-1])
    lines = lax.axis_size("chain") * lax.axis_size("pno")
    last, sums = products(cells**-0.5, mine, theirs, mask, terms, lines)
    sums = lax.all_to_all(sums, ("chain", "pno"), 0, 0, tiled=True)
    sums = jnp.broadcast_to(jnp.sum(sums, axis=0), (lax.axis_size("pair"), 1, width))
    sums = lax.all_to_all(sums, "pair", 0, 0, tiled=True)
    return tuple(finish(sums, own, denom, terms + [last]))


def solution(mesh):
    in_specs = (
        P(("job", "chain", "pair"), "pno", None),
        P(("job", "chain", "pair"), "pno", None),
        P(("job", "chain", "pair"), None, None, None),
        P(("job", "chain", "pair"), None),
        P(("job", "chain", "pair"), None),
        P(("job", "chain", "pair")),
        P(("job", "chain", "pair")),
        P(("job", "chain", "pair"), None),
    )
    out_specs = (P(("job", "chain", "pair"), "pno", None), P("job"))
    return jax.shard_map(
        per_device, mesh=mesh, in_specs=in_specs, out_specs=out_specs, check_vma=False
    )
```
